32 devices in a mesh: owner: 4 (over y, core), rows: 8 (over z, x).
Axes of the slice: x: 2, y: 2, z: 4, core: 2. Of those that a mesh axis runs over, the one named last changes fastest.
Arguments:
- w_gate: float32 [64, 2048, 1024], P('owner', 'rows'), may hold values from -0.1875 to 0.1875
- avg_gate: float32 [64, 2048, 1024], P('owner', 'rows'), may hold values from -0.125 to 0.125
- w_up: float32 [64, 2048, 1024], P('owner', 'rows'), may hold values from -0.1875 to 0.1875
- avg_up: float32 [64, 2048, 1024], P('owner', 'rows'), may hold values from -0.125 to 0.125
- mix_share: float32 [64], P('owner'), may hold values from 0.2 to 0.8
- router_weight: float32 [2048, 64], P('rows', 'owner'), may hold values from -0.125 to 0.125
- router_gain: float32 [2048], P('rows'), may hold values from 0.25 to 1.75
Outputs:
- serve_gate: bfloat16 [64, 2048, 1024], P('owner', None, 'rows')
- serve_up: bfloat16 [64, 2048, 1024], P('owner', None, 'rows')
- scale_gate: float32 [64, 1024], P('owner', 'rows')
- scale_up: float32 [64, 1024], P('owner', 'rows')
- serve_router: bfloat16 [2048, 64], replicated
The draws below stay inside these ranges and needn't reach their ends.
All inputs are finite; a program needn't handle non-finite values.
Results may differ from the reference program's by a relative error of at most 0.001.
Values may be sent and summed in bfloat16 or wider, within the bound.
A program may use at most 256 MiB of HBM per device.

```python
import jax
import jax.numpy as jnp
from jax import lax

EXPERTS = 64
D_MODEL = 2048
D_EXPERT = 1024


def raised(array, key, source, target, parts, factor):
    owner, partner = [(jnp.arange(array.shape[position]) // (array.shape[position] // parts)).reshape([-1 if axis == position else 1 for axis in range(array.ndim)]) for position in (source, target)]
    chosen = jax.random.permutation(key, parts)[partner]
    strong = (owner == chosen) | (owner == (partner + parts // 2) % parts)
    return jnp.where(strong, factor * array, array)


def levels(key, dims, split, smallest, high):
    def one(dim, blocks):
        steps = jax.random.uniform(jax.random.fold_in(jax.random.fold_in(key, 6), dim), (blocks,), jnp.float32, smallest / len(split), high / len(split))
        return jnp.repeat(jnp.exp(steps), dims[dim] // blocks).reshape((-1,) + (1,) * (len(dims) - dim - 1))

    level = one(*split[0])
    for cut in split[1:]:
        level = level * one(*cut)
    return level


def scatter_about(rng, extent, deviation, most, split=(), kind=jnp.bfloat16):
    gain = levels(rng, extent, split, -0.22, 0.18) if split else 1.0
    result = jax.random.normal(rng, extent, jnp.float32) * deviation * gain
    return jnp.minimum(jnp.maximum(result, -most), most).astype(kind)


def noise_with(stream_key, dims, spread, reach, shards, heavy, dtype=jnp.bfloat16):
    entries = spread * jax.random.normal(stream_key, dims, jnp.float32)
    if shards:
        entries = entries * levels(stream_key, dims, shards, -0.22, 0.18)
    return jnp.clip(raised(entries, jax.random.fold_in(stream_key, 3), *heavy), -reach, reach).astype(dtype)


def setup_inputs(seed: int = 0) -> dict:
    seeds = jax.random.split(jax.random.key(seed), 8)
    w_gate = noise_with(seeds[0], (EXPERTS, D_MODEL, D_EXPERT), D_MODEL ** -0.5, 0.1875, ((0, 4), (1, 8)), (1, 2, 8, 2.0), jnp.float32)
    avg_gate = scatter_about(seeds[1], (EXPERTS, D_MODEL, D_EXPERT), D_MODEL ** -0.5, 0.125, ((0, 4), (1, 8)), jnp.float32)
    w_up = noise_with(seeds[2], (EXPERTS, D_MODEL, D_EXPERT), D_MODEL ** -0.5, 0.1875, ((0, 4), (1, 8)), (1, 2, 8, 2.0), jnp.float32)
    avg_up = scatter_about(seeds[3], (EXPERTS, D_MODEL, D_EXPERT), D_MODEL ** -0.5, 0.125, ((0, 4), (1, 8)), jnp.float32)
    mix_share = jnp.clip(0.2 + 0.6 * jax.random.uniform(seeds[4], (EXPERTS,), jnp.float32) ** levels(seeds[4], (EXPERTS,), ((0, 4),), -0.2, 0.2), 0.2, 0.8)
    router_weight = scatter_about(seeds[5], (D_MODEL, EXPERTS), D_MODEL ** -0.5, 0.125, ((0, 8), (1, 4)), jnp.float32)
    router_gain = jnp.clip(1.0 + 0.15 * jax.random.normal(seeds[6], (D_MODEL,), jnp.float32), 0.25, 1.75)
    return dict(w_gate=w_gate, avg_gate=avg_gate, w_up=w_up, avg_up=avg_up, mix_share=mix_share, router_weight=router_weight, router_gain=router_gain)


def reference(w_gate, avg_gate, w_up, avg_up, mix_share, router_weight, router_gain):
    fresh_gate = mix_share[:, None, None] * w_gate + (1.0 - mix_share[:, None, None]) * avg_gate
    fresh_up = mix_share[:, None, None] * w_up + (1.0 - mix_share[:, None, None]) * avg_up
    scale_gate = jnp.sqrt(lax.optimization_barrier(jnp.sum(fresh_gate * fresh_gate, axis=1)))
    serve_gate = (fresh_gate / jnp.expand_dims(scale_gate, 1)).astype(jnp.bfloat16)
    scale_up = jnp.sqrt(lax.optimization_barrier(jnp.sum(fresh_up * fresh_up, axis=1)))
    serve_up = (fresh_up / jnp.expand_dims(scale_up, 1)).astype(jnp.bfloat16)
    serve_router = (router_weight * router_gain[:, None]).astype(jnp.bfloat16)
    return (serve_gate, serve_up, scale_gate, scale_up, serve_router)
```

```python
import functools

import jax
import jax.numpy as jnp
from jax import lax
from jax.experimental import pallas as pl
from jax.experimental.pallas import tpu as pltpu
from jax.sharding import PartitionSpec as P

MESH = pl.DeviceIdType.MESH
LANES = 128
STAGES = 3
STEP = 16
PIECES = 4
HEAD = (4, 4, 2)


def plain(w_gate, avg_gate, w_up, avg_up, mix_share, router_weight, router_gain):
    fresh_gate = mix_share[:, None, None] * w_gate + (1.0 - mix_share[:, None, None]) * avg_gate
    fresh_up = mix_share[:, None, None] * w_up + (1.0 - mix_share[:, None, None]) * avg_up
    total_gate, total_up = lax.psum(
        (jnp.sum(fresh_gate * fresh_gate, axis=1), jnp.sum(fresh_up * fresh_up, axis=1)), "rows"
    )
    scale_gate = jnp.sqrt(total_gate)
    scale_up = jnp.sqrt(total_up)
    narrow_gate, narrow_up = (
        (fresh_gate / jnp.expand_dims(scale_gate, 1)).astype(jnp.bfloat16),
        (fresh_up / jnp.expand_dims(scale_up, 1)).astype(jnp.bfloat16),
    )
    serve_gate, serve_up = (
        lax.all_to_all(narrow_gate, "rows", split_axis=2, concat_axis=1, tiled=True),
        lax.all_to_all(narrow_up, "rows", split_axis=2, concat_axis=1, tiled=True),
    )
    scale_gate = lax.dynamic_slice_in_dim(
        scale_gate, lax.axis_index("rows") * serve_gate.shape[2], serve_gate.shape[2], axis=1
    )
    scale_up = lax.dynamic_slice_in_dim(
        scale_up, lax.axis_index("rows") * serve_up.shape[2], serve_up.shape[2], axis=1
    )
    part_router = (router_weight * router_gain[:, None]).astype(jnp.bfloat16)
    row_router = lax.all_gather(part_router, "rows", axis=0, tiled=True)
    serve_router = lax.all_gather(row_router, "owner", axis=1, tiled=True)
    return (serve_gate, serve_up, scale_gate, scale_up, serve_router)


def kernel(n, owners, wg, ag, wu, au, share, rw, gain,
           og, ou, sg, su, orouter,
           load, fresh, part, gotten, halves, across, held, scales, narrow, rblock,
           load_sem, head_sem, raw_send, raw_recv, rest_send, rest_recv, rs_send, rs_recv, x_send, x_recv, ag_send, ag_recv, b_send, b_recv, own_sem, r_send, r_recv, q_send, q_recv):
    me = lax.axis_index("rows")
    mine = lax.axis_index("owner")
    experts, depth, width = wg.shape
    cols = width // n
    slots = fresh.shape[0]
    outs = (og, ou)
    half = n // 2
    order = tuple(range(half, n)) + tuple(range(half - 1, 0, -1))
    spot = lax.rem(me, half)
    top = 2 * (me // half)
    near = half * (me // half)
    far = half - near
    raws = len(HEAD) - 1
    head = [depth // k for k in HEAD]
    edges = [sum(head[:p]) for p in range(len(head))]
    raw = edges[raws]

    def loads(i, slot):
        return [pltpu.make_async_copy(src.at[i], load.at[slot, j], load_sem.at[slot, j])
                for j, src in enumerate((wg, ag, wu, au))]

    def head_loads(p):
        rows = pl.ds(edges[p], head[p])
        return [pltpu.make_async_copy(src.at[0, rows], load.at[0, j, rows], head_sem.at[p, j])
                for j, src in enumerate((wg, ag, wu, au))]

    def raw_copy(p, m, d):
        peer = me ^ d
        rows = pl.ds(edges[p], head[p])
        there = pl.ds(pl.multiple_of(me * depth + edges[p], STEP), head[p])
        return pltpu.make_async_remote_copy(
            src_ref=narrow.at[m, peer, 0, rows], dst_ref=outs[m].at[0, there, :], send_sem=raw_send, recv_sem=raw_recv,
            device_id={"rows": peer}, device_id_type=MESH)

    def rs_copy(i, d):
        peer = me ^ d
        return pltpu.make_async_remote_copy(
            src_ref=part.at[i, lax.rem(peer, half)], dst_ref=gotten.at[i, d - 1], send_sem=rs_send, recv_sem=rs_recv.at[i],
            device_id={"rows": peer}, device_id_type=MESH)

    def ag_copy(i, d):
        return pltpu.make_async_remote_copy(
            src_ref=held.at[i], dst_ref=scales.at[i, spot], send_sem=ag_send, recv_sem=ag_recv.at[i],
            device_id={"rows": me ^ d}, device_id_type=MESH)

    def cross_copy(i):
        return pltpu.make_async_remote_copy(
            src_ref=halves.at[i], dst_ref=across.at[i], send_sem=x_send, recv_sem=x_recv.at[i],
            device_id={"rows": me ^ half}, device_id_type=MESH)

    def bulk_copy(i, m, d):
        peer = me ^ d
        return pltpu.make_async_remote_copy(
            src_ref=narrow.at[m, peer, i], dst_ref=outs[m].at[i, pl.ds(me * depth, depth), :],
            send_sem=b_send.at[m, d - 1], recv_sem=b_recv.at[m, d - 1],
            device_id={"rows": peer}, device_id_type=MESH)

    def rest_copy(m, d):
        peer = me ^ d
        there = pl.ds(pl.multiple_of(me * depth + raw, STEP), depth - raw)
        return pltpu.make_async_remote_copy(
            src_ref=narrow.at[m, peer, 0, pl.ds(raw, depth - raw)], dst_ref=outs[m].at[0, there, :],
            send_sem=rest_send, recv_sem=rest_recv,
            device_id={"rows": peer}, device_id_type=MESH)

    def own_copy(i, m):
        return pltpu.make_async_copy(
            narrow.at[m, me, i], outs[m].at[i, pl.ds(me * depth, depth), :], own_sem.at[m])

    for p in range(len(HEAD)):
        for copy in head_loads(p):
            copy.start()

    barrier = pltpu.get_barrier_semaphore()
    for d in range(1, n):
        pl.semaphore_signal(barrier, inc=1, device_id={"rows": me ^ d}, device_id_type=MESH)
    for q in range(1, owners):
        pl.semaphore_signal(barrier, inc=1, device_id={"owner": mine ^ q}, device_id_type=MESH)

    rexp, rlen = rw.shape
    rrows = pl.ds(pl.multiple_of(mine * rexp, rexp), rexp)
    rcols = pl.ds(pl.multiple_of(me * rlen, LANES), rlen)
    rblock[...] = (rw[...] * gain[...]).astype(jnp.bfloat16)

    def router_copy(d):
        return pltpu.make_async_remote_copy(
            src_ref=rblock, dst_ref=orouter.at[rrows, rcols], send_sem=r_send.at[d - 1], recv_sem=r_recv,
            device_id={"rows": me ^ d}, device_id_type=MESH)

    def router_across(q):
        return pltpu.make_async_remote_copy(
            src_ref=orouter.at[rrows, :], dst_ref=orouter.at[rrows, :], send_sem=q_send.at[q - 1],
            recv_sem=q_recv.at[q - 1], device_id={"owner": mine ^ q}, device_id_type=MESH)

    orouter[rrows, rcols] = rblock[...]

    def blend(i, slot, fslot, m, lo, hi, acc, ship=False):
        a = share[i]
        b = 1.0 - a

        def rows_step(t, acc):
            rows = pl.ds(pl.multiple_of(t * STEP, STEP), STEP)
            f = a * load[slot, 2 * m, rows, :] + b * load[slot, 2 * m + 1, rows, :]
            fresh[fslot, m, rows, :] = f
            f = f * f
            for r in range(0, STEP, 8):
                acc = acc + f[r:r + 8]
            if ship:
                for j in range(half):
                    c = far + j
                    g = fresh[fslot, m, rows, pl.ds(pl.multiple_of(c * cols, LANES), cols)]
                    narrow[m, c, 0, rows, :] = g.astype(jnp.bfloat16)
            return acc
        return lax.fori_loop(lo // STEP, hi // STEP, rows_step, acc)

    def sums(i, m, acc):
        total = jnp.sum(acc, axis=0, keepdims=True)
        for c in range(n):
            part[i, c % half, pl.ds(2 * (c // half) + m, 1), :] = total[:, c * cols:(c + 1) * cols]

    def mix(i):
        slot = lax.rem(i, 2)
        for copy in loads(i, slot):
            copy.wait()
        for m in range(2):
            sums(i, m, blend(i, slot, lax.rem(i, slots), m, 0, depth, jnp.zeros((8, width), jnp.float32)))

        @pl.when(i + 2 < experts)
        def _():
            for copy in loads(i + 2, slot):
                copy.start()

    def ship(p):
        for d in order:
            if d >= half:
                for m in range(2):
                    raw_copy(p, m, d).start()

    def spread(i):
        for d in range(half - 1, 0, -1):
            rs_copy(i, d).start()

    def halve(i):
        pltpu.make_async_copy(gotten.at[i], gotten.at[i], rs_recv.at[i]).wait()
        total = part[i, spot]
        for d in range(half - 1):
            total = total + gotten[i, d]
        halves[i] = total
        cross_copy(i).start()

    def settle(i):
        cross_copy(i).wait_recv()
        scale = jnp.sqrt(halves[i] + across[i])
        held[i] = scale
        scales[i, spot] = scale
        sg[pl.ds(i, 1), :] = held[i, pl.ds(top, 1), :]
        su[pl.ds(i, 1), :] = held[i, pl.ds(top + 1, 1), :]
        for d in range(half - 1, 0, -1):
            ag_copy(i, d).start()

    def send(i):
        fslot = lax.rem(i, slots)
        landed = scales.at[i, pl.ds(0, half - 1)]
        pltpu.make_async_copy(landed, landed, ag_recv.at[i]).wait()
        for m in range(2):
            inverse = [1.0 / scales[i, c % half, pl.ds(2 * (c // half) + m, 1), :] for c in range(n)]

            def rows_step(t, carry):
                rows = pl.ds(pl.multiple_of(t * STEP, STEP), STEP)
                for c in range(n):
                    f = fresh[fslot, m, rows, c * cols:(c + 1) * cols]
                    narrow[m, c, i, rows, :] = (f * inverse[c]).astype(jnp.bfloat16)
                return carry
            lax.fori_loop(0, depth // STEP, rows_step, 0)
        for d in order:
            for m in range(2):
                bulk_copy(i, m, d).start()
        for m in range(2):
            own_copy(i, m).start()

    def scaled(i, m, c, rows, col, inverse):
        f = fresh[lax.rem(i, slots), m, rows, pl.ds(col, cols)]
        narrow[m, c, i, rows, :] = (f * inverse).astype(jnp.bfloat16)

    def send_first():
        landed = scales.at[0, pl.ds(0, half - 1)]
        pltpu.make_async_copy(landed, landed, ag_recv.at[0]).wait()
        for m in range(2):
            def near_step(t, carry):
                rows = pl.ds(pl.multiple_of(t * STEP, STEP), STEP)
                for j in range(half):
                    c = near + j
                    scaled(0, m, c, rows, pl.multiple_of(c * cols, LANES), 1.0 / scales[0, j, pl.ds(top + m, 1), :])
                return carry
            lax.fori_loop(0, raw // STEP, near_step, 0)

            def rows_step(t, carry):
                rows = pl.ds(pl.multiple_of(t * STEP, STEP), STEP)
                for c in range(n):
                    scaled(0, m, c, rows, c * cols, 1.0 / scales[0, c % half, pl.ds(2 * (c // half) + m, 1), :])
                return carry
            lax.fori_loop(raw // STEP, depth // STEP, rows_step, 0)
        for d in order:
            for m in range(2):
                if d < half:
                    bulk_copy(0, m, d).start()
                else:
                    rest_copy(m, d).start()
        for m in range(2):
            own_copy(0, m).start()

    def turn(i, carry):
        @pl.when(i < experts)
        def _():
            mix(i)
            spread(i)

        @pl.when(i <= experts)
        def _():
            halve(i - 1)

        @pl.when(i == 1)
        def _():
            for p in range(1, raws):
                ship(p)
            for d in order:
                router_copy(d).start()

        @pl.when((i >= 2) & (i <= experts + 1))
        def _():
            settle(i - 2)

        @pl.when(i == STAGES)
        def _():
            send_first()

        @pl.when(i > STAGES)
        def _():
            send(i - STAGES)
        return carry

    accs = [jnp.zeros((8, width), jnp.float32)] * 2
    for p in range(len(HEAD)):
        for copy in head_loads(p):
            copy.wait()
        accs = [blend(0, 0, 0, m, edges[p], edges[p] + head[p], accs[m], p < raws) for m in range(2)]
        if p == 0:
            for copy in loads(1, 1):
                copy.start()
            pl.semaphore_wait(barrier, n + owners - 2)
            ship(0)
    for m in range(2):
        sums(0, m, accs[m])
    spread(0)
    for copy in loads(2, 0):
        copy.start()
    lax.fori_loop(1, experts + STAGES, turn, 0)

    early = og.at[0, pl.ds(0, 2 * half * raw), :]
    pltpu.make_async_copy(early, early, raw_recv).wait()
    for m in range(2):
        inverse = 1.0 / held[0, pl.ds(top + m, 1), :]

        def fix(t, carry):
            for j in range(half):
                rows = pl.ds(pl.multiple_of((far + j) * depth + t * STEP, STEP), STEP)
                outs[m][0, rows, :] = (outs[m][0, rows, :].astype(jnp.float32) * inverse).astype(jnp.bfloat16)
            return carry
        lax.fori_loop(0, raw // STEP, fix, 0)

    got = orouter.at[rrows, pl.ds(0, (n - 1) * rlen)]
    pltpu.make_async_copy(got, got, r_recv).wait()
    for q in range(1, owners):
        router_across(q).start()
    for d in range(1, n):
        router_copy(d).wait_send()
    for m in range(2):
        block = outs[m].at[:, pl.ds(0, depth), :]
        pltpu.make_async_copy(block, block, own_sem.at[m]).wait()
        most = outs[m].at[pl.ds(0, experts - 1), pl.ds(0, depth), :]
        for d in range(1, n):
            sent = block if d < half else most
            pltpu.make_async_copy(sent, sent, b_send.at[m, d - 1]).wait()
            pltpu.make_async_copy(sent, sent, b_recv.at[m, d - 1]).wait()
    pltpu.make_async_copy(early, early, raw_send).wait()
    rest = og.at[0, pl.ds(0, 2 * half * (depth - raw)), :]
    pltpu.make_async_copy(rest, rest, rest_send).wait()
    pltpu.make_async_copy(rest, rest, rest_recv).wait()
    pltpu.make_async_copy(gotten, gotten, rs_send).wait()
    pltpu.make_async_copy(across, across, x_send).wait()
    every = scales.at[:, pl.ds(0, half - 1)]
    pltpu.make_async_copy(every, every, ag_send).wait()
    for q in range(1, owners):
        router_across(q).wait()


def flush(*refs):
    sources, targets, sem = refs[:len(refs) // 2], refs[len(refs) // 2:-1], refs[-1]
    copies = []
    for source, target in zip(sources, targets):
        pieces = PIECES if len(source.shape) == 3 else 1
        size = source.shape[0] // pieces
        for p in range(pieces):
            block = pl.ds(p * size, size)
            copies.append(pltpu.make_async_copy(source.at[block], target.at[block], sem.at[len(copies)]))
    for copy in copies:
        copy.start()
    for copy in copies:
        copy.wait()


def body(n, owners, w_gate, avg_gate, w_up, avg_up, mix_share, router_weight, router_gain):
    experts, depth, width = w_gate.shape
    cols = width // n
    rlen, rexp = router_weight.shape
    f32, bf16 = jnp.float32, jnp.bfloat16
    dma = pltpu.SemaphoreType.DMA
    hbm = pl.BlockSpec(memory_space=pl.ANY)
    vmem = pl.BlockSpec(memory_space=pltpu.VMEM)
    smem = pl.BlockSpec(memory_space=pltpu.SMEM)
    landed = pl.pallas_call(
        functools.partial(kernel, n, owners),
        out_shape=(
            OUT((experts, n * depth, cols), bf16),
            OUT((experts, n * depth, cols), bf16),
            OUT((experts, cols), f32),
            OUT((experts, cols), f32),
            OUT((owners * rexp, n * rlen), bf16),
        ),
        in_specs=[hbm] * 4 + [smem, vmem, vmem],
        out_specs=(OUT_SPEC, OUT_SPEC, vmem, vmem, vmem),
        scratch_shapes=[
            pltpu.VMEM((2, 4, depth, width), f32),
            pltpu.VMEM((STAGES + 1, 2, depth, width), f32),
            pltpu.VMEM((experts, n // 2, 4, cols), f32),
            pltpu.VMEM((experts, n // 2 - 1, 4, cols), f32),
            pltpu.VMEM((experts, 4, cols), f32),
            pltpu.VMEM((experts, 4, cols), f32),
            pltpu.VMEM((experts, 4, cols), f32),
            pltpu.VMEM((experts, n // 2, 4, cols), f32),
            pltpu.VMEM((2, n, experts, depth, cols), bf16),
            pltpu.VMEM((rexp, rlen), bf16),
            dma((2, 4)), dma((len(HEAD), 4)), dma, dma, dma, dma, dma, dma((experts,)), dma, dma((experts,)), dma, dma((experts,)),
            dma((2, n - 1)), dma((2, n - 1)), dma((2,)),
            dma((n - 1,)), dma, dma((owners - 1,)), dma((owners - 1,)),
        ],
        compiler_params=pltpu.CompilerParams(
            collective_id=0, has_side_effects=True, vmem_limit_bytes=LIMIT
        ),
    )(w_gate, avg_gate, w_up, avg_up, mix_share, router_weight.T, router_gain[None, :])
    serve_gate, serve_up, scale_gate, scale_up, router = pl.pallas_call(
        flush,
        out_shape=[pltpu.HBM(x.shape, x.dtype) for x in landed],
        in_specs=[vmem] * len(landed),
        out_specs=[pl.BlockSpec(memory_space=pltpu.HBM)] * len(landed),
        scratch_shapes=[dma((len(landed) + 2 * (PIECES - 1),))],
        compiler_params=pltpu.CompilerParams(vmem_limit_bytes=1024 * 1024),
    )(*landed)
    return serve_gate, serve_up, scale_gate, scale_up, router.T


OUT = pltpu.VMEM
OUT_SPEC = pl.BlockSpec(memory_space=pltpu.VMEM)
LIMIT = 44 * 1024 * 1024


def fits(mesh, w_gate, router_weight):
    n, owners = mesh.shape["rows"], mesh.shape["owner"]
    experts, depth, width = w_gate.shape[0] // owners, w_gate.shape[1] // n, w_gate.shape[2]
    head = [depth // k for k in HEAD]
    half_raw = n // 2 * sum(head[:-1])
    need = 4 * depth * width * (8 + 2 * (STAGES + 1)) + 4 * experts * depth * width
    return (
        n > 2 and owners > 1 and n & (n - 1) == 0 and owners & (owners - 1) == 0
        and width % (n * LANES) == 0 and depth % LANES == 0 and depth % STEP == 0
        and experts % 16 == 0 and (router_weight.shape[1] // owners) % 16 == 0
        and depth == sum(head) and head[0] % STEP == 0 and 64 * half_raw <= experts * depth * n and need < 40 * 1024 * 1024
    )


def solution(mesh):
    in_specs = (
        P("owner", "rows", None),
        P("owner", "rows", None),
        P("owner", "rows", None),
        P("owner", "rows", None),
        P("owner"),
        P("rows", "owner"),
        P("rows"),
    )
    out_specs = (
        P("owner", None, "rows"),
        P("owner", None, "rows"),
        P("owner", "rows"),
        P("owner", "rows"),
        P(),
    )

    def call(w_gate, avg_gate, w_up, avg_up, mix_share, router_weight, router_gain):
        inner = plain
        if fits(mesh, w_gate, router_weight):
            inner = functools.partial(body, mesh.shape["rows"], mesh.shape["owner"])
        step = jax.shard_map(inner, mesh=mesh, in_specs=in_specs, out_specs=out_specs, check_vma=False)
        return step(w_gate, avg_gate, w_up, avg_up, mix_share, router_weight, router_gain)

    return call
```

```python
import functools

import jax
import jax.numpy as jnp
from jax import lax
from jax.experimental import pallas as pl
from jax.experimental.pallas import tpu as pltpu
from jax.sharding import PartitionSpec as P

MESH = pl.DeviceIdType.MESH
LANES = 128
SLOTS = 5
LEAD = 2
STEP = 16
PIECES = 4
HEAD = (8, 8, 4, 2)


def plain(w_gate, avg_gate, w_up, avg_up, mix_share, router_weight, router_gain):
    fresh_gate = mix_share[:, None, None] * w_gate + (1.0 - mix_share[:, None, None]) * avg_gate
    fresh_up = mix_share[:, None, None] * w_up + (1.0 - mix_share[:, None, None]) * avg_up
    total_gate, total_up = lax.psum(
        (jnp.sum(fresh_gate * fresh_gate, axis=1), jnp.sum(fresh_up * fresh_up, axis=1)), "rows"
    )
    scale_gate = jnp.sqrt(total_gate)
    scale_up = jnp.sqrt(total_up)
    narrow_gate, narrow_up = (
        (fresh_gate / jnp.expand_dims(scale_gate, 1)).astype(jnp.bfloat16),
        (fresh_up / jnp.expand_dims(scale_up, 1)).astype(jnp.bfloat16),
    )
    serve_gate, serve_up = (
        lax.all_to_all(narrow_gate, "rows", split_axis=2, concat_axis=1, tiled=True),
        lax.all_to_all(narrow_up, "rows", split_axis=2, concat_axis=1, tiled=True),
    )
    scale_gate = lax.dynamic_slice_in_dim(
        scale_gate, lax.axis_index("rows") * serve_gate.shape[2], serve_gate.shape[2], axis=1
    )
    scale_up = lax.dynamic_slice_in_dim(
        scale_up, lax.axis_index("rows") * serve_up.shape[2], serve_up.shape[2], axis=1
    )
    part_router = (router_weight * router_gain[:, None]).astype(jnp.bfloat16)
    row_router = lax.all_gather(part_router, "rows", axis=0, tiled=True)
    serve_router = lax.all_gather(row_router, "owner", axis=1, tiled=True)
    return (serve_gate, serve_up, scale_gate, scale_up, serve_router)


def kernel(n, owners, wg, ag, wu, au, share_in, rw_in, gain_in,
           og, ou, sg, su, orouter,
           load, fresh, part, gotten, halves, across, held, scales, narrow, rblock, share, rw, gain,
           small_sem, load_sem, head_sem, raw_send, raw_recv, rest_send, rest_recv, rs_send, rs_recv, x_send, x_recv, ag_send, ag_recv, b_send, b_recv, own_sem, r_send, r_recv, f_send, f_recv, q_send, q_recv):
    me = lax.axis_index("rows")
    mine = lax.axis_index("owner")
    experts, depth, width = wg.shape
    cols = width // n
    slots = fresh.shape[0]
    outs = (og, ou)
    half = n // 2
    order = tuple(range(half, n)) + tuple(range(half - 1, 0, -1))
    spot = lax.rem(me, half)
    top = 2 * (me // half)
    near = half * (me // half)
    far = half - near
    raws = len(HEAD) - 1
    head = [depth // k for k in HEAD]
    edges = [sum(head[:p]) for p in range(len(head))]
    raw = edges[raws]

    def loads(i, slot):
        return [pltpu.make_async_copy(src.at[i], load.at[slot, j], load_sem.at[slot, j])
                for j, src in enumerate((wg, ag, wu, au))]

    def head_loads(p):
        rows = pl.ds(edges[p], head[p])
        return [pltpu.make_async_copy(src.at[0, rows], load.at[0, j, rows], head_sem.at[p, j])
                for j, src in enumerate((wg, ag, wu, au))]

    def raw_copy(p, m, d):
        peer = me ^ d
        rows = pl.ds(edges[p], head[p])
        there = pl.ds(pl.multiple_of(me * depth + edges[p], STEP), head[p])
        return pltpu.make_async_remote_copy(
            src_ref=narrow.at[m, peer, 0, rows], dst_ref=outs[m].at[0, there, :], send_sem=raw_send, recv_sem=raw_recv,
            device_id={"rows": peer}, device_id_type=MESH)

    def rs_copy(i, d):
        peer = me ^ d
        return pltpu.make_async_remote_copy(
            src_ref=part.at[i, lax.rem(peer, half)], dst_ref=gotten.at[i, d - 1], send_sem=rs_send, recv_sem=rs_recv.at[i],
            device_id={"rows": peer}, device_id_type=MESH)

    def ag_copy(i, d):
        return pltpu.make_async_remote_copy(
            src_ref=held.at[i], dst_ref=scales.at[i, spot], send_sem=ag_send, recv_sem=ag_recv.at[i],
            device_id={"rows": me ^ d}, device_id_type=MESH)

    def cross_copy(i, count):
        block = pl.ds(i, count)
        return pltpu.make_async_remote_copy(
            src_ref=halves.at[block], dst_ref=across.at[block], send_sem=x_send, recv_sem=x_recv.at[i],
            device_id={"rows": me ^ half}, device_id_type=MESH)

    def bulk_copy(i, m, d):
        peer = me ^ d
        return pltpu.make_async_remote_copy(
            src_ref=narrow.at[m, peer, i], dst_ref=outs[m].at[i, pl.ds(me * depth, depth), :],
            send_sem=b_send.at[m, d - 1], recv_sem=b_recv.at[m, d - 1],
            device_id={"rows": peer}, device_id_type=MESH)

    def rest_copy(m, d):
        peer = me ^ d
        there = pl.ds(pl.multiple_of(me * depth + raw, STEP), depth - raw)
        return pltpu.make_async_remote_copy(
            src_ref=narrow.at[m, peer, 0, pl.ds(raw, depth - raw)], dst_ref=outs[m].at[0, there, :],
            send_sem=rest_send, recv_sem=rest_recv,
            device_id={"rows": peer}, device_id_type=MESH)

    def own_copy(i, m):
        return pltpu.make_async_copy(
            narrow.at[m, me, i], outs[m].at[i, pl.ds(me * depth, depth), :], own_sem.at[m])

    smalls = [pltpu.make_async_copy(src, dst, small_sem.at[j])
              for j, (src, dst) in enumerate(((share_in, share), (rw_in, rw), (gain_in, gain)))]
    smalls[0].start()
    for p in range(len(HEAD)):
        for copy in head_loads(p):
            copy.start()
    for copy in smalls[1:]:
        copy.start()

    barrier = pltpu.get_barrier_semaphore()
    for d in range(1, n):
        pl.semaphore_signal(barrier, inc=1, device_id={"rows": me ^ d}, device_id_type=MESH)
    for q in range(1, owners):
        pl.semaphore_signal(barrier, inc=1, device_id={"owner": mine ^ q}, device_id_type=MESH)

    rexp, rlen = rw_in.shape
    rrows = pl.ds(pl.multiple_of(mine * rexp, rexp), rexp)
    rcols = pl.ds(pl.multiple_of(me * rlen, LANES), rlen)

    def router_copy(d):
        return pltpu.make_async_remote_copy(
            src_ref=rblock, dst_ref=orouter.at[rrows, rcols], send_sem=r_send, recv_sem=r_recv.at[d // half],
            device_id={"rows": me ^ d}, device_id_type=MESH)

    def router_forward(d):
        block = orouter.at[rrows, pl.ds(pl.multiple_of((me ^ half) * rlen, LANES), rlen)]
        return pltpu.make_async_remote_copy(
            src_ref=block, dst_ref=block, send_sem=f_send, recv_sem=f_recv,
            device_id={"rows": me ^ d}, device_id_type=MESH)

    def router_across(q):
        return pltpu.make_async_remote_copy(
            src_ref=orouter.at[rrows, :], dst_ref=orouter.at[rrows, :], send_sem=q_send.at[q - 1],
            recv_sem=q_recv.at[q - 1], device_id={"owner": mine ^ q}, device_id_type=MESH)

    def gate_rows():
        for copy in smalls[1:]:
            copy.wait()
        rblock[...] = (rw[...] * gain[...]).astype(jnp.bfloat16)
        orouter[rrows, rcols] = rblock[...]

    def blend(i, slot, fslot, m, lo, hi, acc, ship=False):
        a = share[i]
        b = 1.0 - a

        def rows_step(t, acc):
            rows = pl.ds(pl.multiple_of(t * STEP, STEP), STEP)
            f = a * load[slot, 2 * m, rows, :] + b * load[slot, 2 * m + 1, rows, :]
            fresh[fslot, m, rows, :] = f
            f = f * f
            for r in range(0, STEP, 8):
                acc = acc + f[r:r + 8]
            if ship:
                for j in range(half):
                    c = far + j
                    g = fresh[fslot, m, rows, pl.ds(pl.multiple_of(c * cols, LANES), cols)]
                    narrow[m, c, 0, rows, :] = g.astype(jnp.bfloat16)
            return acc
        return lax.fori_loop(lo // STEP, hi // STEP, rows_step, acc)

    def sums(i, m, acc):
        total = jnp.sum(acc, axis=0, keepdims=True)
        for c in range(n):
            part[i, c % half, pl.ds(2 * (c // half) + m, 1), :] = total[:, c * cols:(c + 1) * cols]

    def mix(i):
        slot = lax.rem(i, 2)
        for copy in loads(i, slot):
            copy.wait()
        for m in range(2):
            sums(i, m, blend(i, slot, lax.rem(i, slots), m, 0, depth, jnp.zeros((8, width), jnp.float32)))

        @pl.when(i + 2 < experts)
        def _():
            for copy in loads(i + 2, slot):
                copy.start()

    def ship(p):
        for m in range(2):
            for d in range(half, n):
                raw_copy(p, m, d).start()

    def spread(i):
        for d in range(half - 1, 0, -1):
            rs_copy(i, d).start()

    def halve(i):
        pltpu.make_async_copy(gotten.at[i], gotten.at[i], rs_recv.at[i]).wait()
        total = part[i, spot]
        for d in range(half - 1):
            total = total + gotten[i, d]
        halves[i] = total

        @pl.when(i < LEAD)
        def _():
            cross_copy(i, 1).start()

        @pl.when((i >= LEAD) & (lax.rem(i, 2) == 1))
        def _():
            cross_copy(i - 1, 2).start()

    def settle(i):
        @pl.when(i < LEAD)
        def _():
            cross_copy(i, 1).wait_recv()

        @pl.when((i >= LEAD) & (lax.rem(i, 2) == 0))
        def _():
            cross_copy(i, 2).wait_recv()
        scale = jnp.sqrt(halves[i] + across[i])
        held[i] = scale
        scales[i, spot] = scale
        sg[pl.ds(i, 1), :] = held[i, pl.ds(top, 1), :]
        su[pl.ds(i, 1), :] = held[i, pl.ds(top + 1, 1), :]
        for d in range(half - 1, 0, -1):
            ag_copy(i, d).start()

    def send(i):
        fslot = lax.rem(i, slots)
        landed = scales.at[i, pl.ds(0, half - 1)]
        pltpu.make_async_copy(landed, landed, ag_recv.at[i]).wait()
        for m in range(2):
            inverse = [1.0 / scales[i, c % half, pl.ds(2 * (c // half) + m, 1), :] for c in range(n)]

            def rows_step(t, carry):
                rows = pl.ds(pl.multiple_of(t * STEP, STEP), STEP)
                for c in range(n):
                    f = fresh[fslot, m, rows, c * cols:(c + 1) * cols]
                    narrow[m, c, i, rows, :] = (f * inverse[c]).astype(jnp.bfloat16)
                return carry
            lax.fori_loop(0, depth // STEP, rows_step, 0)
            for d in order:
                bulk_copy(i, m, d).start()
            own_copy(i, m).start()

    def scaled(i, m, c, rows, col, inverse):
        f = fresh[lax.rem(i, slots), m, rows, pl.ds(col, cols)]
        narrow[m, c, i, rows, :] = (f * inverse).astype(jnp.bfloat16)

    def send_first():
        landed = scales.at[0, pl.ds(0, half - 1)]
        pltpu.make_async_copy(landed, landed, ag_recv.at[0]).wait()
        for m in range(2):
            def near_step(t, carry):
                rows = pl.ds(pl.multiple_of(t * STEP, STEP), STEP)
                for j in range(half):
                    c = near + j
                    scaled(0, m, c, rows, pl.multiple_of(c * cols, LANES), 1.0 / scales[0, j, pl.ds(top + m, 1), :])
                return carry
            lax.fori_loop(0, raw // STEP, near_step, 0)

            def rows_step(t, carry):
                rows = pl.ds(pl.multiple_of(t * STEP, STEP), STEP)
                for c in range(n):
                    scaled(0, m, c, rows, c * cols, 1.0 / scales[0, c % half, pl.ds(2 * (c // half) + m, 1), :])
                return carry
            lax.fori_loop(raw // STEP, depth // STEP, rows_step, 0)
            for d in order:
                (bulk_copy(0, m, d) if d < half else rest_copy(m, d)).start()
            own_copy(0, m).start()

    def turn(i, carry):
        @pl.when(i < experts)
        def _():
            mix(i)
            spread(i)

        @pl.when(i <= experts)
        def _():
            halve(i - 1)

        @pl.when(i == 1)
        def _():
            for p in range(1, raws):
                ship(p)
            gate_rows()
            for d in range(half, 0, -1):
                router_copy(d).start()

        @pl.when((i >= 2) & (i < LEAD + 2))
        def _():
            settle(i - 2)

        @pl.when((i >= LEAD + 3) & (i <= experts + 2))
        def _():
            settle(i - 3)

        @pl.when(i == 3)
        def _():
            send_first()

        @pl.when((i > 3) & (i < LEAD + 3))
        def _():
            send(i - 3)

        @pl.when(i >= LEAD + 4)
        def _():
            send(i - 4)

        @pl.when(i == LEAD + 4)
        def _():
            got = orouter.at[rrows, pl.ds(0, rlen)]
            pltpu.make_async_copy(got, got, r_recv.at[1]).wait()
            for d in range(half - 1, 0, -1):
                router_forward(d).start()
        return carry

    smalls[0].wait()
    accs = [jnp.zeros((8, width), jnp.float32)] * 2
    for p in range(len(HEAD)):
        for copy in head_loads(p):
            copy.wait()
        accs = [blend(0, 0, 0, m, edges[p], edges[p] + head[p], accs[m], p < raws) for m in range(2)]
        if p == 0:
            for copy in loads(1, 1):
                copy.start()
            pl.semaphore_wait(barrier, n + owners - 2)
            ship(0)
    for m in range(2):
        sums(0, m, accs[m])
    spread(0)
    for copy in loads(2, 0):
        copy.start()
    lax.fori_loop(1, experts + 4, turn, 0)

    early = og.at[0, pl.ds(0, 2 * half * raw), :]
    pltpu.make_async_copy(early, early, raw_recv).wait()
    for m in range(2):
        inverse = 1.0 / held[0, pl.ds(top + m, 1), :]

        def fix(t, carry):
            for j in range(half):
                rows = pl.ds(pl.multiple_of((far + j) * depth + t * STEP, STEP), STEP)
                outs[m][0, rows, :] = (outs[m][0, rows, :].astype(jnp.float32) * inverse).astype(jnp.bfloat16)
            return carry
        lax.fori_loop(0, raw // STEP, fix, 0)

    got = orouter.at[rrows, pl.ds(0, (half - 1) * rlen)]
    pltpu.make_async_copy(got, got, r_recv.at[0]).wait()
    pltpu.make_async_copy(got, got, f_recv).wait()
    for q in range(1, owners):
        router_across(q).start()
    sent = orouter.at[rrows, pl.ds(0, half * rlen)]
    pltpu.make_async_copy(sent, sent, r_send).wait()
    pltpu.make_async_copy(got, got, f_send).wait()
    for m in range(2):
        block = outs[m].at[:, pl.ds(0, depth), :]
        pltpu.make_async_copy(block, block, own_sem.at[m]).wait()
        most = outs[m].at[pl.ds(0, experts - 1), pl.ds(0, depth), :]
        for d in range(1, n):
            sent = block if d < half else most
            pltpu.make_async_copy(sent, sent, b_send.at[m, d - 1]).wait()
            pltpu.make_async_copy(sent, sent, b_recv.at[m, d - 1]).wait()
    pltpu.make_async_copy(early, early, raw_send).wait()
    rest = og.at[0, pl.ds(0, 2 * half * (depth - raw)), :]
    pltpu.make_async_copy(rest, rest, rest_send).wait()
    pltpu.make_async_copy(rest, rest, rest_recv).wait()
    pltpu.make_async_copy(gotten, gotten, rs_send).wait()
    pltpu.make_async_copy(across, across, x_send).wait()
    every = scales.at[:, pl.ds(0, half - 1)]
    pltpu.make_async_copy(every, every, ag_send).wait()
    for q in range(1, owners):
        router_across(q).wait()


def flush(*refs):
    sources, targets, sem = refs[:len(refs) // 2], refs[len(refs) // 2:-1], refs[-1]
    copies = []
    for source, target in zip(sources, targets):
        pieces = PIECES if len(source.shape) == 3 else 1
        size = source.shape[0] // pieces
        for p in range(pieces):
            block = pl.ds(p * size, size)
            copies.append(pltpu.make_async_copy(source.at[block], target.at[block], sem.at[len(copies)]))
    for copy in copies:
        copy.start()
    for copy in copies:
        copy.wait()


def body(n, owners, w_gate, avg_gate, w_up, avg_up, mix_share, router_weight, router_gain):
    experts, depth, width = w_gate.shape
    cols = width // n
    rlen, rexp = router_weight.shape
    f32, bf16 = jnp.float32, jnp.bfloat16
    dma = pltpu.SemaphoreType.DMA
    hbm = pl.BlockSpec(memory_space=pl.ANY)
    vmem = pl.BlockSpec(memory_space=pltpu.VMEM)
    landed = pl.pallas_call(
        functools.partial(kernel, n, owners),
        out_shape=(
            OUT((experts, n * depth, cols), bf16),
            OUT((experts, n * depth, cols), bf16),
            OUT((experts, cols), f32),
            OUT((experts, cols), f32),
            OUT((owners * rexp, n * rlen), bf16),
        ),
        in_specs=[hbm] * 7,
        out_specs=(OUT_SPEC, OUT_SPEC, vmem, vmem, vmem),
        scratch_shapes=[
            pltpu.VMEM((2, 4, depth, width), f32),
            pltpu.VMEM((SLOTS, 2, depth, width), f32),
            pltpu.VMEM((experts, n // 2, 4, cols), f32),
            pltpu.VMEM((experts, n // 2 - 1, 4, cols), f32),
            pltpu.VMEM((experts, 4, cols), f32),
            pltpu.VMEM((experts, 4, cols), f32),
            pltpu.VMEM((experts, 4, cols), f32),
            pltpu.VMEM((experts, n // 2, 4, cols), f32),
            pltpu.VMEM((2, n, experts, depth, cols), bf16),
            pltpu.VMEM((rexp, rlen), bf16),
            pltpu.SMEM((experts,), f32),
            pltpu.VMEM((rexp, rlen), f32),
            pltpu.VMEM((1, rlen), f32),
            dma((3,)), dma((2, 4)), dma((len(HEAD), 4)), dma, dma, dma, dma, dma, dma((experts,)), dma, dma((experts,)), dma, dma((experts,)),
            dma((2, n - 1)), dma((2, n - 1)), dma((2,)),
            dma, dma((2,)), dma, dma, dma((owners - 1,)), dma((owners - 1,)),
        ],
        compiler_params=pltpu.CompilerParams(
            collective_id=0, has_side_effects=True, vmem_limit_bytes=LIMIT
        ),
    )(w_gate, avg_gate, w_up, avg_up, mix_share, router_weight.T, router_gain[None, :])
    serve_gate, serve_up, scale_gate, scale_up, router = pl.pallas_call(
        flush,
        out_shape=[pltpu.HBM(x.shape, x.dtype) for x in landed],
        in_specs=[vmem] * len(landed),
        out_specs=[pl.BlockSpec(memory_space=pltpu.HBM)] * len(landed),
        scratch_shapes=[dma((len(landed) + 2 * (PIECES - 1),))],
        compiler_params=pltpu.CompilerParams(vmem_limit_bytes=1024 * 1024),
    )(*landed)
    return serve_gate, serve_up, scale_gate, scale_up, router.T


OUT = pltpu.VMEM
OUT_SPEC = pl.BlockSpec(memory_space=pltpu.VMEM)
LIMIT = 46 * 1024 * 1024


def fits(mesh, w_gate, router_weight):
    n, owners = mesh.shape["rows"], mesh.shape["owner"]
    experts, depth, width = w_gate.shape[0] // owners, w_gate.shape[1] // n, w_gate.shape[2]
    head = [depth // k for k in HEAD]
    half_raw = n // 2 * sum(head[:-1])
    need = 4 * depth * width * (8 + 2 * SLOTS) + 4 * experts * depth * width
    return (
        n > 2 and owners > 1 and n & (n - 1) == 0 and owners & (owners - 1) == 0
        and width % (n * LANES) == 0 and depth % LANES == 0 and depth % STEP == 0
        and experts % 16 == 0 and (router_weight.shape[1] // owners) % 16 == 0
        and depth == sum(head) and head[0] % STEP == 0 and 64 * half_raw <= experts * depth * n and need < 40 * 1024 * 1024
    )


def solution(mesh):
    in_specs = (
        P("owner", "rows", None),
        P("owner", "rows", None),
        P("owner", "rows", None),
        P("owner", "rows", None),
        P("owner"),
        P("rows", "owner"),
        P("rows"),
    )
    out_specs = (
        P("owner", None, "rows"),
        P("owner", None, "rows"),
        P("owner", "rows"),
        P("owner", "rows"),
        P(),
    )

    def call(w_gate, avg_gate, w_up, avg_up, mix_share, router_weight, router_gain):
        inner = plain
        if fits(mesh, w_gate, router_weight):
            inner = functools.partial(body, mesh.shape["rows"], mesh.shape["owner"])
        step = jax.shard_map(inner, mesh=mesh, in_specs=in_specs, out_specs=out_specs, check_vma=False)
        return step(w_gate, avg_gate, w_up, avg_up, mix_share, router_weight, router_gain)

    return call
```

```python
import functools

import jax
import jax.numpy as jnp
from jax import lax
from jax.experimental import pallas as pl
from jax.experimental.pallas import tpu as pltpu
from jax.sharding import PartitionSpec as P

MESH = pl.DeviceIdType.MESH
LANES = 128
SLOTS = 5
LEAD = 2
STEP = 16
PIECES = 4
HEAD = (8, 8, 8, 8, 2)
INNER = (0, 1, 6, 6)
OUTER = (6, 6, 7, 7)


def plain(w_gate, avg_gate, w_up, avg_up, mix_share, router_weight, router_gain):
    fresh_gate = mix_share[:, None, None] * w_gate + (1.0 - mix_share[:, None, None]) * avg_gate
    fresh_up = mix_share[:, None, None] * w_up + (1.0 - mix_share[:, None, None]) * avg_up
    total_gate, total_up = lax.psum(
        (jnp.sum(fresh_gate * fresh_gate, axis=1), jnp.sum(fresh_up * fresh_up, axis=1)), "rows"
    )
    scale_gate = jnp.sqrt(total_gate)
    scale_up = jnp.sqrt(total_up)
    narrow_gate, narrow_up = (
        (fresh_gate / jnp.expand_dims(scale_gate, 1)).astype(jnp.bfloat16),
        (fresh_up / jnp.expand_dims(scale_up, 1)).astype(jnp.bfloat16),
    )
    serve_gate, serve_up = (
        lax.all_to_all(narrow_gate, "rows", split_axis=2, concat_axis=1, tiled=True),
        lax.all_to_all(narrow_up, "rows", split_axis=2, concat_axis=1, tiled=True),
    )
    scale_gate = lax.dynamic_slice_in_dim(
        scale_gate, lax.axis_index("rows") * serve_gate.shape[2], serve_gate.shape[2], axis=1
    )
    scale_up = lax.dynamic_slice_in_dim(
        scale_up, lax.axis_index("rows") * serve_up.shape[2], serve_up.shape[2], axis=1
    )
    part_router = (router_weight * router_gain[:, None]).astype(jnp.bfloat16)
    row_router = lax.all_gather(part_router, "rows", axis=0, tiled=True)
    serve_router = lax.all_gather(row_router, "owner", axis=1, tiled=True)
    return (serve_gate, serve_up, scale_gate, scale_up, serve_router)


def kernel(n, owners, wg, ag, wu, au, share_in, rw_in, gain_in,
           og, ou, sg, su, orouter,
           load, fresh, part, gotten, halves, across, held, scales, narrow, rblock, share, rw, gain,
           small_sem, load_sem, head_sem, raw_send, raw_recv, rest_send, rest_recv, rs_send, rs_recv, x_send, x_recv, ag_send, ag_recv, b_send, b_recv, own_sem, r_send, r_recv, f_send, f_recv, q_send, q_recv):
    me = lax.axis_index("rows")
    mine = lax.axis_index("owner")
    experts, depth, width = wg.shape
    cols = width // n
    slots = fresh.shape[0]
    outs = (og, ou)
    half = n // 2
    order = tuple(range(half, n)) + tuple(range(half - 1, 0, -1))
    spot = lax.rem(me, half)
    top = 2 * (me // half)
    near = half * (me // half)
    far = half - near
    inner = (me // half) != (2 * me // half) % 2
    raws = len(HEAD) - 1
    head = [depth // k for k in HEAD]
    edges = [sum(head[:p]) for p in range(len(head))]
    raw = edges[raws]

    def loads(i, slot):
        return [pltpu.make_async_copy(src.at[i], load.at[slot, j], load_sem.at[slot, j])
                for j, src in enumerate((wg, ag, wu, au))]

    def head_loads(p):
        rows = pl.ds(edges[p], head[p])
        return [pltpu.make_async_copy(src.at[0, rows], load.at[0, j, rows], head_sem.at[p, j])
                for j, src in enumerate((wg, ag, wu, au))]

    def raw_copy(p, m, d):
        peer = me ^ d
        rows = pl.ds(edges[p], head[p])
        there = pl.ds(pl.multiple_of(me * depth + edges[p], STEP), head[p])
        return pltpu.make_async_remote_copy(
            src_ref=narrow.at[m, peer, 0, rows], dst_ref=outs[m].at[0, there, :], send_sem=raw_send, recv_sem=raw_recv,
            device_id={"rows": peer}, device_id_type=MESH)

    def rs_copy(i, d):
        peer = me ^ d
        return pltpu.make_async_remote_copy(
            src_ref=part.at[i, lax.rem(peer, half)], dst_ref=gotten.at[i, d - 1], send_sem=rs_send, recv_sem=rs_recv.at[i],
            device_id={"rows": peer}, device_id_type=MESH)

    def ag_copy(i, d):
        return pltpu.make_async_remote_copy(
            src_ref=held.at[i], dst_ref=scales.at[i, spot], send_sem=ag_send, recv_sem=ag_recv.at[i],
            device_id={"rows": me ^ d}, device_id_type=MESH)

    def cross_copy(i, count):
        block = pl.ds(i, count)
        return pltpu.make_async_remote_copy(
            src_ref=halves.at[block], dst_ref=across.at[block], send_sem=x_send, recv_sem=x_recv.at[i],
            device_id={"rows": me ^ half}, device_id_type=MESH)

    def bulk_copy(i, m, d):
        peer = me ^ d
        return pltpu.make_async_remote_copy(
            src_ref=narrow.at[m, peer, i], dst_ref=outs[m].at[i, pl.ds(me * depth, depth), :],
            send_sem=b_send.at[m, d - 1], recv_sem=b_recv.at[m, d - 1],
            device_id={"rows": peer}, device_id_type=MESH)

    def rest_copy(m, d):
        peer = me ^ d
        there = pl.ds(pl.multiple_of(me * depth + raw, STEP), depth - raw)
        return pltpu.make_async_remote_copy(
            src_ref=narrow.at[m, peer, 0, pl.ds(raw, depth - raw)], dst_ref=outs[m].at[0, there, :],
            send_sem=rest_send, recv_sem=rest_recv,
            device_id={"rows": peer}, device_id_type=MESH)

    def own_copy(i, m):
        return pltpu.make_async_copy(
            narrow.at[m, me, i], outs[m].at[i, pl.ds(me * depth, depth), :], own_sem.at[m])

    smalls = [pltpu.make_async_copy(src, dst, small_sem.at[j])
              for j, (src, dst) in enumerate(((share_in, share), (rw_in, rw), (gain_in, gain)))]
    smalls[0].start()
    for p in range(len(HEAD)):
        for copy in head_loads(p):
            copy.start()
    for copy in smalls[1:]:
        copy.start()

    barrier = pltpu.get_barrier_semaphore()
    for d in range(1, n):
        pl.semaphore_signal(barrier, inc=1, device_id={"rows": me ^ d}, device_id_type=MESH)
    for q in range(1, owners):
        pl.semaphore_signal(barrier, inc=1, device_id={"owner": mine ^ q}, device_id_type=MESH)

    rexp, rlen = rw_in.shape
    rrows = pl.ds(pl.multiple_of(mine * rexp, rexp), rexp)
    rcols = pl.ds(pl.multiple_of(me * rlen, LANES), rlen)

    def router_copy(d):
        return pltpu.make_async_remote_copy(
            src_ref=rblock, dst_ref=orouter.at[rrows, rcols], send_sem=r_send, recv_sem=r_recv.at[d // half],
            device_id={"rows": me ^ d}, device_id_type=MESH)

    def router_forward(d):
        block = orouter.at[rrows, pl.ds(pl.multiple_of((me ^ half) * rlen, LANES), rlen)]
        return pltpu.make_async_remote_copy(
            src_ref=block, dst_ref=block, send_sem=f_send, recv_sem=f_recv,
            device_id={"rows": me ^ d}, device_id_type=MESH)

    def router_across(q):
        return pltpu.make_async_remote_copy(
            src_ref=orouter.at[rrows, :], dst_ref=orouter.at[rrows, :], send_sem=q_send.at[q - 1],
            recv_sem=q_recv.at[q - 1], device_id={"owner": mine ^ q}, device_id_type=MESH)

    def gate_rows():
        for copy in smalls[1:]:
            copy.wait()
        rblock[...] = (rw[...] * gain[...]).astype(jnp.bfloat16)
        orouter[rrows, rcols] = rblock[...]

    def blend(i, slot, fslot, m, lo, hi, acc, ship=False):
        a = share[i]
        b = 1.0 - a

        def rows_step(t, acc):
            rows = pl.ds(pl.multiple_of(t * STEP, STEP), STEP)
            f = a * load[slot, 2 * m, rows, :] + b * load[slot, 2 * m + 1, rows, :]
            fresh[fslot, m, rows, :] = f
            f = f * f
            for r in range(0, STEP, 8):
                acc = acc + f[r:r + 8]
            if ship:
                for j in range(half):
                    c = far + j
                    g = fresh[fslot, m, rows, pl.ds(pl.multiple_of(c * cols, LANES), cols)]
                    narrow[m, c, 0, rows, :] = g.astype(jnp.bfloat16)
            return acc
        return lax.fori_loop(lo // STEP, hi // STEP, rows_step, acc)

    def sums(i, m, acc):
        total = jnp.sum(acc, axis=0, keepdims=True)
        for c in range(n):
            part[i, c % half, pl.ds(2 * (c // half) + m, 1), :] = total[:, c * cols:(c + 1) * cols]

    def mix(i):
        slot = lax.rem(i, 2)
        for copy in loads(i, slot):
            copy.wait()
        for m in range(2):
            sums(i, m, blend(i, slot, lax.rem(i, slots), m, 0, depth, jnp.zeros((8, width), jnp.float32)))

        @pl.when(i + 2 < experts)
        def _():
            for copy in loads(i + 2, slot):
                copy.start()

    def ship(point):
        for here, points in ((inner, INNER), (~inner, OUTER)):
            parts = [p for p in range(raws) if points[p] == point]
            if parts:
                @pl.when(here)
                def _():
                    for p in parts:
                        for m in range(2):
                            for d in range(half, n):
                                raw_copy(p, m, d).start()

    def spread(i):
        for d in range(half - 1, 0, -1):
            rs_copy(i, d).start()

    def halve(i):
        pltpu.make_async_copy(gotten.at[i], gotten.at[i], rs_recv.at[i]).wait()
        total = part[i, spot]
        for d in range(half - 1):
            total = total + gotten[i, d]
        halves[i] = total

        @pl.when(i < LEAD)
        def _():
            cross_copy(i, 1).start()

        @pl.when((i >= LEAD) & (lax.rem(i, 2) == 1))
        def _():
            cross_copy(i - 1, 2).start()

    def settle(i):
        @pl.when(i < LEAD)
        def _():
            cross_copy(i, 1).wait_recv()

        @pl.when((i >= LEAD) & (lax.rem(i, 2) == 0))
        def _():
            cross_copy(i, 2).wait_recv()
        scale = jnp.sqrt(halves[i] + across[i])
        held[i] = scale
        scales[i, spot] = scale
        sg[pl.ds(i, 1), :] = held[i, pl.ds(top, 1), :]
        su[pl.ds(i, 1), :] = held[i, pl.ds(top + 1, 1), :]
        for d in range(half - 1, 0, -1):
            ag_copy(i, d).start()

    def send(i):
        fslot = lax.rem(i, slots)
        landed = scales.at[i, pl.ds(0, half - 1)]
        pltpu.make_async_copy(landed, landed, ag_recv.at[i]).wait()
        for m in range(2):
            inverse = [1.0 / scales[i, c % half, pl.ds(2 * (c // half) + m, 1), :] for c in range(n)]

            def rows_step(t, carry):
                rows = pl.ds(pl.multiple_of(t * STEP, STEP), STEP)
                for c in range(n):
                    f = fresh[fslot, m, rows, c * cols:(c + 1) * cols]
                    narrow[m, c, i, rows, :] = (f * inverse[c]).astype(jnp.bfloat16)
                return carry
            lax.fori_loop(0, depth // STEP, rows_step, 0)
            for d in order:
                bulk_copy(i, m, d).start()
            own_copy(i, m).start()

    def scaled(i, m, c, rows, col, inverse):
        f = fresh[lax.rem(i, slots), m, rows, pl.ds(col, cols)]
        narrow[m, c, i, rows, :] = (f * inverse).astype(jnp.bfloat16)

    def send_first():
        landed = scales.at[0, pl.ds(0, half - 1)]
        pltpu.make_async_copy(landed, landed, ag_recv.at[0]).wait()
        for m in range(2):
            def near_step(t, carry):
                rows = pl.ds(pl.multiple_of(t * STEP, STEP), STEP)
                for j in range(half):
                    c = near + j
                    scaled(0, m, c, rows, pl.multiple_of(c * cols, LANES), 1.0 / scales[0, j, pl.ds(top + m, 1), :])
                return carry
            lax.fori_loop(0, raw // STEP, near_step, 0)

            def rows_step(t, carry):
                rows = pl.ds(pl.multiple_of(t * STEP, STEP), STEP)
                for c in range(n):
                    scaled(0, m, c, rows, c * cols, 1.0 / scales[0, c % half, pl.ds(2 * (c // half) + m, 1), :])
                return carry
            lax.fori_loop(raw // STEP, depth // STEP, rows_step, 0)
            for d in order:
                (bulk_copy(0, m, d) if d < half else rest_copy(m, d)).start()
            own_copy(0, m).start()

    def turn(i, carry):
        @pl.when(i < experts)
        def _():
            mix(i)
            spread(i)

        @pl.when(i <= experts)
        def _():
            halve(i - 1)

        @pl.when(i == 1)
        def _():
            ship(len(HEAD) + 1)
            gate_rows()
            for d in range(half, 0, -1):
                router_copy(d).start()

        @pl.when((i >= 2) & (i < LEAD + 2))
        def _():
            settle(i - 2)

        @pl.when(i == 2)
        def _():
            ship(len(HEAD) + 2)

        @pl.when((i >= LEAD + 3) & (i <= experts + 2))
        def _():
            settle(i - 3)

        @pl.when(i == 3)
        def _():
            send_first()

        @pl.when((i > 3) & (i < LEAD + 3))
        def _():
            send(i - 3)

        @pl.when(i >= LEAD + 4)
        def _():
            send(i - 4)

        @pl.when(i == LEAD + 4)
        def _():
            got = orouter.at[rrows, pl.ds(0, rlen)]
            pltpu.make_async_copy(got, got, r_recv.at[1]).wait()
            for d in range(half - 1, 0, -1):
                router_forward(d).start()
        return carry

    smalls[0].wait()
    accs = [jnp.zeros((8, width), jnp.float32)] * 2
    for p in range(len(HEAD)):
        for copy in head_loads(p):
            copy.wait()
        accs = [blend(0, 0, 0, m, edges[p], edges[p] + head[p], accs[m], p < raws) for m in range(2)]
        if p == 0:
            for copy in loads(1, 1):
                copy.start()
            pl.semaphore_wait(barrier, n + owners - 2)
        ship(p)
    for m in range(2):
        sums(0, m, accs[m])
    spread(0)
    ship(len(HEAD))
    for copy in loads(2, 0):
        copy.start()
    lax.fori_loop(1, experts + 4, turn, 0)

    early = og.at[0, pl.ds(0, 2 * half * raw), :]
    pltpu.make_async_copy(early, early, raw_recv).wait()
    for m in range(2):
        inverse = 1.0 / held[0, pl.ds(top + m, 1), :]

        def fix(t, carry):
            for j in range(half):
                rows = pl.ds(pl.multiple_of((far + j) * depth + t * STEP, STEP), STEP)
                outs[m][0, rows, :] = (outs[m][0, rows, :].astype(jnp.float32) * inverse).astype(jnp.bfloat16)
            return carry
        lax.fori_loop(0, raw // STEP, fix, 0)

    got = orouter.at[rrows, pl.ds(0, (half - 1) * rlen)]
    pltpu.make_async_copy(got, got, r_recv.at[0]).wait()
    pltpu.make_async_copy(got, got, f_recv).wait()
    for q in range(1, owners):
        router_across(q).start()
    sent = orouter.at[rrows, pl.ds(0, half * rlen)]
    pltpu.make_async_copy(sent, sent, r_send).wait()
    pltpu.make_async_copy(got, got, f_send).wait()
    for m in range(2):
        block = outs[m].at[:, pl.ds(0, depth), :]
        pltpu.make_async_copy(block, block, own_sem.at[m]).wait()
        most = outs[m].at[pl.ds(0, experts - 1), pl.ds(0, depth), :]
        for d in range(1, n):
            sent = block if d < half else most
            pltpu.make_async_copy(sent, sent, b_send.at[m, d - 1]).wait()
            pltpu.make_async_copy(sent, sent, b_recv.at[m, d - 1]).wait()
    pltpu.make_async_copy(early, early, raw_send).wait()
    rest = og.at[0, pl.ds(0, 2 * half * (depth - raw)), :]
    pltpu.make_async_copy(rest, rest, rest_send).wait()
    pltpu.make_async_copy(rest, rest, rest_recv).wait()
    pltpu.make_async_copy(gotten, gotten, rs_send).wait()
    pltpu.make_async_copy(across, across, x_send).wait()
    every = scales.at[:, pl.ds(0, half - 1)]
    pltpu.make_async_copy(every, every, ag_send).wait()
    for q in range(1, owners):
        router_across(q).wait()


def flush(*refs):
    sources, targets, sem = refs[:len(refs) // 2], refs[len(refs) // 2:-1], refs[-1]
    copies = []
    for source, target in zip(sources, targets):
        pieces = PIECES if len(source.shape) == 3 else 1
        size = source.shape[0] // pieces
        for p in range(pieces):
            block = pl.ds(p * size, size)
            copies.append(pltpu.make_async_copy(source.at[block], target.at[block], sem.at[len(copies)]))
    for copy in copies:
        copy.start()
    for copy in copies:
        copy.wait()


def body(n, owners, w_gate, avg_gate, w_up, avg_up, mix_share, router_weight, router_gain):
    experts, depth, width = w_gate.shape
    cols = width // n
    rlen, rexp = router_weight.shape
    f32, bf16 = jnp.float32, jnp.bfloat16
    dma = pltpu.SemaphoreType.DMA
    hbm = pl.BlockSpec(memory_space=pl.ANY)
    vmem = pl.BlockSpec(memory_space=pltpu.VMEM)
    landed = pl.pallas_call(
        functools.partial(kernel, n, owners),
        out_shape=(
            OUT((experts, n * depth, cols), bf16),
            OUT((experts, n * depth, cols), bf16),
            OUT((experts, cols), f32),
            OUT((experts, cols), f32),
            OUT((owners * rexp, n * rlen), bf16),
        ),
        in_specs=[hbm] * 7,
        out_specs=(OUT_SPEC, OUT_SPEC, vmem, vmem, vmem),
        scratch_shapes=[
            pltpu.VMEM((2, 4, depth, width), f32),
            pltpu.VMEM((SLOTS, 2, depth, width), f32),
            pltpu.VMEM((experts, n // 2, 4, cols), f32),
            pltpu.VMEM((experts, n // 2 - 1, 4, cols), f32),
            pltpu.VMEM((experts, 4, cols), f32),
            pltpu.VMEM((experts, 4, cols), f32),
            pltpu.VMEM((experts, 4, cols), f32),
            pltpu.VMEM((experts, n // 2, 4, cols), f32),
            pltpu.VMEM((2, n, experts, depth, cols), bf16),
            pltpu.VMEM((rexp, rlen), bf16),
            pltpu.SMEM((experts,), f32),
            pltpu.VMEM((rexp, rlen), f32),
            pltpu.VMEM((1, rlen), f32),
            dma((3,)), dma((2, 4)), dma((len(HEAD), 4)), dma, dma, dma, dma, dma, dma((experts,)), dma, dma((experts,)), dma, dma((experts,)),
            dma((2, n - 1)), dma((2, n - 1)), dma((2,)),
            dma, dma((2,)), dma, dma, dma((owners - 1,)), dma((owners - 1,)),
        ],
        compiler_params=pltpu.CompilerParams(
            collective_id=0, has_side_effects=True, vmem_limit_bytes=LIMIT
        ),
    )(w_gate, avg_gate, w_up, avg_up, mix_share, router_weight.T, router_gain[None, :])
    serve_gate, serve_up, scale_gate, scale_up, router = pl.pallas_call(
        flush,
        out_shape=[pltpu.HBM(x.shape, x.dtype) for x in landed],
        in_specs=[vmem] * len(landed),
        out_specs=[pl.BlockSpec(memory_space=pltpu.HBM)] * len(landed),
        scratch_shapes=[dma((len(landed) + 2 * (PIECES - 1),))],
        compiler_params=pltpu.CompilerParams(vmem_limit_bytes=1024 * 1024),
    )(*landed)
    return serve_gate, serve_up, scale_gate, scale_up, router.T


OUT = pltpu.VMEM
OUT_SPEC = pl.BlockSpec(memory_space=pltpu.VMEM)
LIMIT = 46 * 1024 * 1024


def fits(mesh, w_gate, router_weight):
    n, owners = mesh.shape["rows"], mesh.shape["owner"]
    experts, depth, width = w_gate.shape[0] // owners, w_gate.shape[1] // n, w_gate.shape[2]
    head = [depth // k for k in HEAD]
    half_raw = n // 2 * sum(head[:-1])
    need = 4 * depth * width * (8 + 2 * SLOTS) + 4 * experts * depth * width
    return (
        n > 2 and owners > 1 and n & (n - 1) == 0 and owners & (owners - 1) == 0
        and width % (n * LANES) == 0 and depth % LANES == 0 and depth % STEP == 0
        and experts % 16 == 0 and (router_weight.shape[1] // owners) % 16 == 0
        and depth == sum(head) and head[0] % STEP == 0 and 64 * half_raw <= experts * depth * n and need < 40 * 1024 * 1024
    )


def solution(mesh):
    in_specs = (
        P("owner", "rows", None),
        P("owner", "rows", None),
        P("owner", "rows", None),
        P("owner", "rows", None),
        P("owner"),
        P("rows", "owner"),
        P("rows"),
    )
    out_specs = (
        P("owner", None, "rows"),
        P("owner", None, "rows"),
        P("owner", "rows"),
        P("owner", "rows"),
        P(),
    )

    def call(w_gate, avg_gate, w_up, avg_up, mix_share, router_weight, router_gain):
        inner = plain
        if fits(mesh, w_gate, router_weight):
            inner = functools.partial(body, mesh.shape["rows"], mesh.shape["owner"])
        step = jax.shard_map(inner, mesh=mesh, in_specs=in_specs, out_specs=out_specs, check_vma=False)
        return step(w_gate, avg_gate, w_up, avg_up, mix_share, router_weight, router_gain)

    return call
```
